1024 devices in a mesh: dp: 64 (over y_hi, z, core), ctx: 16 (over x, y_lo).
Axes of the slice: x: 8, y: 8 (y_hi: 4, y_lo: 2; y = y_hi * 2 + y_lo), z: 8, core: 2. Of those that a mesh axis runs over, the one named last changes fastest.
Arguments:
- qkv: bfloat16 [64, 2048, 5120], P('dp', 'ctx'), may hold values from -8 to 8
- dest: int32 [64, 32], P('dp'), may hold values from 0 to 63, as said below
- order: int32 [32], replicated, may hold values from 0 to 31, as said below
- lengths: int32 [64, 8], replicated, may hold values from 1 to 1024, 2048 in all within a row
Outputs:
- attended: bfloat16 [64, 2048, 4096], P('dp', 'ctx')
The draws below stay inside these ranges and needn't reach their ends.
Inputs may be any that keep to these rules, and one draw needn't show every extreme that they name: `dest`: entry [r, s] is r itself, r + 1 or r - 1 (indices modulo 64), and the relation is mutual: if entry [r, s] is t, entry [t, s] is r. For every c below 16: order[2 c] is below 16 and order[2 c + 1] = 31 - order[2 c]; every span appears once.
All inputs are finite; a program needn't handle non-finite values.
Results may differ from the reference program's by a relative error of at most 0.0031.
Values may be sent and summed in bfloat16 or wider, within the bound.
No kernel may reach another device: no remote copies, remote signals or barrier semaphores. Data moves between devices by JAX's collectives and lax.ppermute only.
A program may use at most 64 MiB of HBM per device.

```python
import math
import jax
import jax.numpy as jnp
import numpy as np
from jax import lax

QUERY_HEADS = 32
KEY_VALUE_HEADS = 4
HEAD_SIZE = 128
NDOC = 8
SPAN = 64
QUERIES_PER_KV = 8
WIDTH = 5120
PACKED_LENGTH = 2048
MAXDOC = 1024
PACKED_COUNT = 64
N_CTX = 16


def draw_dest(key, part):
    parity = jax.random.randint(jax.random.fold_in(key, 11), (2 * N_CTX,), 0, 2)
    flips = jax.random.randint(jax.random.fold_in(key, 12), (PACKED_COUNT, 2 * N_CTX), 0, 2)
    ranks = jnp.arange(PACKED_COUNT, dtype=jnp.int32)[:, None]
    is_lower = (ranks - parity[None, :]) % 2 == 0
    lower_member = jnp.where(is_lower, ranks, ranks - 1) % PACKED_COUNT
    partner = jnp.where(is_lower, ranks + 1, ranks - 1) % PACKED_COUNT
    traded = jnp.take_along_axis(flips, lower_member, axis=0)
    return jnp.where(traded == 1, partner, ranks * jnp.ones_like(partner)).astype(jnp.int32)


def draw_order(key, part):
    early = jax.random.permutation(jax.random.fold_in(key, 21), N_CTX).astype(jnp.int32)
    late = (2 * N_CTX - 1 - early).astype(jnp.int32)
    return jnp.stack([early, late], axis=1).reshape(2 * N_CTX).astype(jnp.int32)


def draw_qkv(key, part):
    random_keys = jax.random.split(jax.random.fold_in(key, 31), 1)
    blank_scores = jax.random.normal(random_keys[0], (PACKED_COUNT, PACKED_LENGTH, WIDTH), jnp.float32)
    return jnp.clip(blank_scores, -8.0, 8.0).astype(jnp.bfloat16)


def profile(number_of, total, most, skew):
    weights = [(1 << 20) // math.isqrt(rank ** skew) + 1 for rank in range(2, number_of + 1)]
    surplus, counts = total - most - (number_of - 1), [1] * (number_of - 1)
    while surplus > 0:
        free = [i for i in range(number_of - 1) if counts[i] < most]
        pool, left = sum([weights[i] for i in free]), surplus
        for i in free:
            addition = min(most - counts[i], max(1, left * weights[i] // pool), surplus)
            counts[i] = counts[i] + addition
            surplus = surplus - addition
    return np.array([most] + counts)


def uneven_parts(own_key, amount, total, limit, lean):
    if amount == 2:
        one = jax.random.randint(own_key, (), max(1, total - limit), min(limit, total - 1) + 1)
        return jnp.stack([one, total - one])
    sizes = jnp.asarray(profile(amount, total, limit, lean), jnp.int32)
    pairs = (amount - 1) // 2
    donor, taker = sizes[1:1 + 2 * pairs:2], sizes[2:2 + 2 * pairs:2]
    slack = jnp.minimum(donor - 1, limit - taker)
    passed = jax.random.randint(jax.random.fold_in(own_key, 1), (pairs,), 0, 1 << 20) % (slack + 1)
    sizes = sizes.at[1:1 + 2 * pairs:2].set(donor - passed).at[2:2 + 2 * pairs:2].set(taker + passed)
    return sizes[jax.random.permutation(jax.random.fold_in(own_key, 2), amount)]


def setup_inputs(seed: int = 0) -> dict:
    streams_of = jax.random.split(jax.random.key(seed), 5)
    qkv = draw_qkv(jax.random.fold_in(streams_of[4], 71), 0)
    dest = draw_dest(jax.random.fold_in(streams_of[4], 71), 0)
    order = draw_order(jax.random.fold_in(streams_of[4], 71), 0)
    lengths = jax.vmap(lambda own: uneven_parts(own, NDOC, PACKED_LENGTH, MAXDOC, 2))(jax.random.split(streams_of[3], PACKED_COUNT)).reshape((PACKED_COUNT, NDOC)).astype(jnp.int32)
    return dict(qkv=qkv, dest=dest, order=order, lengths=lengths)


MASK_FLOOR = -1e+30

def sequence_attention(qkv, dest, order, doc_ends, seq_index):
    row_ids = jnp.arange(PACKED_LENGTH, dtype=jnp.int32)
    row_slot = (row_ids // SPAN).astype(jnp.int32)
    dest_row = lax.dynamic_index_in_dim(dest, seq_index, 0, keepdims=False)
    row_source = jnp.take(dest_row, row_slot).astype(jnp.int32)
    settled = qkv[row_source, row_ids]
    positions = (jnp.take(order, row_slot) * SPAN + row_ids % SPAN).astype(jnp.int32)
    row_ends = jnp.take(doc_ends, row_source, axis=0)
    counted = lax.optimization_barrier(jnp.sum((row_ends <= positions[:, None]).astype(jnp.int32), axis=1))
    documents = (row_source * NDOC + counted).astype(jnp.int32)
    visible = (documents[None, :] == documents[:, None]) & (positions[None, :] <= positions[:, None])
    score_scale = 1.0 / math.sqrt(HEAD_SIZE)
    finished = []
    for head_group_index in range(KEY_VALUE_HEADS):
        query_cols = settled[:, head_group_index * QUERIES_PER_KV * HEAD_SIZE:(head_group_index + 1) * QUERIES_PER_KV * HEAD_SIZE]
        query_block = query_cols.reshape(PACKED_LENGTH, QUERIES_PER_KV, HEAD_SIZE).astype(jnp.float32)
        key_start = QUERY_HEADS * HEAD_SIZE + head_group_index * HEAD_SIZE
        value_offset = (QUERY_HEADS + KEY_VALUE_HEADS) * HEAD_SIZE + head_group_index * HEAD_SIZE
        key_block = settled[:, key_start:key_start + HEAD_SIZE].astype(jnp.float32)
        value_block = settled[:, value_offset:value_offset + HEAD_SIZE].astype(jnp.float32)
        scores = jnp.einsum('qgd,kd->gqk', query_block, key_block, precision=lax.Precision.HIGHEST) * score_scale
        scores = jnp.where(visible[None], scores, MASK_FLOOR)
        row_max = lax.optimization_barrier(jnp.max(scores, axis=2, keepdims=True))
        weights = jnp.where(visible[None], jnp.exp(scores - row_max), 0.0)
        totals = lax.optimization_barrier(jnp.sum(weights, axis=2, keepdims=True))
        rounded = weights.astype(jnp.bfloat16).astype(jnp.float32)
        mixed = jnp.einsum('gqk,kd->gqd', rounded, value_block, precision=lax.Precision.HIGHEST) / totals
        finished.append(jnp.transpose(mixed, (1, 0, 2)).reshape(PACKED_LENGTH, QUERIES_PER_KV * HEAD_SIZE))
    return jnp.concatenate(finished, axis=1).astype(jnp.bfloat16)

def reference(qkv, dest, order, lengths):
    doc_ends = jnp.cumsum(lengths, axis=1).astype(jnp.int32)

    def one_sequence(seq_index):
        return sequence_attention(qkv, dest, order, doc_ends, seq_index)
    return lax.map(one_sequence, jnp.arange(PACKED_COUNT, dtype=jnp.int32))
```

```python
import functools
import math

import jax
import jax.numpy as jnp
from jax import lax
from jax.experimental import pallas as pl
from jax.experimental.pallas import tpu as pltpu
from jax.sharding import Mesh
from jax.sharding import PartitionSpec as P

QUERY_HEADS = 32
KEY_VALUE_HEADS = 4
HEAD_SIZE = 128
NDOC = 8
SPAN = 64
QUERIES_PER_KV = 8
CTX = ("ctx_0", "ctx_1")
QUERY_WIDTH = QUERY_HEADS * HEAD_SIZE
HALF_WIDTH = KEY_VALUE_HEADS * HEAD_SIZE
SPANS = 32
CHUNK = 4
LIST = 40
FAR = 1 << 20
MASK_FLOOR = -1e30
EXP2_SCALE = math.log2(math.e) / math.sqrt(HEAD_SIZE)


def attention_kernel(pieces, count, *refs):
    where_ref, dest_ref, order_ref, lengths_ref = refs[:4]
    query_refs = refs[4:7]
    piece_refs = refs[7 : 7 + count]
    out_ref = refs[7 + count]
    (
        queries,
        keys,
        values,
        listed,
        bases,
        totals_listed,
        ends,
        peaks,
        sums,
        mixed,
        query_sems,
        piece_sems,
    ) = refs[8 + count :]
    rank, column, row = where_ref[0], where_ref[1], where_ref[2]
    sign = 1 - 2 * (column & 1)
    own_slot = 2 * (2 * column + row)
    even_partner = where_ref[3]
    odd_partner = where_ref[4]

    def query_copy(half, which):
        rows = pl.ds(half * SPAN, SPAN)
        return pltpu.make_async_copy(
            query_refs[which].at[rows, pl.ds(0, QUERY_WIDTH)],
            queries.at[half],
            query_sems.at[half],
        )

    sources, spans, firsts = [], [], []
    for half in range(2):
        source = dest_ref[0, own_slot + half]
        for which, partner in enumerate((rank, even_partner, odd_partner)):

            @pl.when(source == partner)
            def _(half=half, which=which):
                query_copy(half, which).start()

        span = order_ref[own_slot + half]
        end, first = jnp.int32(0), jnp.int32(0)
        for doc in range(NDOC):
            end = end + lengths_ref[source, doc]
            ends[half, doc] = end
            first = jnp.where(end <= span * SPAN, end, first)
        sources.append(source)
        spans.append(span)
        firsts.append(first)

    def piece_copies(index):
        ref, first_row = pieces[index][0], pieces[index][1]
        rows = pl.ds(first_row, SPAN)
        there = pl.ds(index * SPAN, SPAN)
        return (
            pltpu.make_async_copy(
                piece_refs[ref].at[rows, pl.ds(0, HALF_WIDTH)], keys.at[there], piece_sems.at[index, 0]
            ),
            pltpu.make_async_copy(
                piece_refs[ref].at[rows, pl.ds(HALF_WIDTH, HALF_WIDTH)],
                values.at[there],
                piece_sems.at[index, 1],
            ),
        )

    counts = [jnp.int32(0), jnp.int32(0)]
    wanted = []
    for index, (_, _, step, flip, part) in enumerate(pieces):
        there = (column + sign * step) & 7
        slot = 2 * (2 * there + (row ^ flip)) + part
        source, span = dest_ref[0, slot], order_ref[slot]
        either = None
        for half in range(2):
            need = (
                (source == sources[half])
                & (span <= spans[half])
                & (span * SPAN + SPAN > firsts[half])
            )

            @pl.when(need)
            def _(half=half, index=index, span=span, at=counts[half]):
                listed[half, at] = index
                bases[half, at] = span * SPAN

            counts[half] = counts[half] + need.astype(jnp.int32)
            either = need if either is None else either | need
        wanted.append(either)

        @pl.when(either)
        def _(index=index):
            for copy in piece_copies(index):
                copy.start()

    for half in range(2):
        totals_listed[half] = (counts[half] + CHUNK - 1) // CHUNK
        for extra in range(CHUNK - 1):
            listed[half, counts[half] + extra] = half
            bases[half, counts[half] + extra] = FAR
        query_copy(half, 0).wait()
    for index in range(SPANS):

        @pl.when(wanted[index])
        def _(index=index):
            for copy in piece_copies(index):
                copy.wait()

    lane = lax.broadcasted_iota(jnp.int32, (1, CHUNK * SPAN), 1)

    def one_half(half, unused):
        position = order_ref[own_slot + half] * SPAN + lax.broadcasted_iota(jnp.int32, (SPAN, 1), 0)
        start = jnp.zeros((SPAN, 1), jnp.int32)
        for doc in range(NDOC):
            end = ends[half, doc]
            start = jnp.where(position >= end, end, start)

        def one_chunk(chunk, opening):
            at = chunk * CHUNK
            key_position = lane & (SPAN - 1)
            base = jnp.full((1, CHUNK * SPAN), bases[half, at], jnp.int32)
            for j in range(1, CHUNK):
                base = jnp.where(lane >= j * SPAN, bases[half, at + j], base)
            key_position = key_position + base
            visible = (key_position <= position) & (key_position >= start)
            bias = jnp.where(visible, 0.0, MASK_FLOOR).astype(jnp.float32)
            firsts_of = [pl.multiple_of(listed[half, at + j] * SPAN, SPAN) for j in range(CHUNK)]
            for group in range(KEY_VALUE_HEADS):
                columns = slice(group * HEAD_SIZE, (group + 1) * HEAD_SIZE)
                key = jnp.concatenate([keys[pl.ds(f, SPAN), columns] for f in firsts_of], axis=0)
                value = jnp.concatenate([values[pl.ds(f, SPAN), columns] for f in firsts_of], axis=0)
                query = jnp.concatenate(
                    [
                        queries[half, :, pl.ds((group * QUERIES_PER_KV + h) * HEAD_SIZE, HEAD_SIZE)]
                        for h in range(QUERIES_PER_KV)
                    ],
                    axis=0,
                )
                score = lax.dot_general(
                    query, key, (((1,), (1,)), ((), ())), preferred_element_type=jnp.float32
                )
                score = score.reshape(QUERIES_PER_KV, SPAN, CHUNK * SPAN) * EXP2_SCALE + bias[None]
                score = score.reshape(QUERIES_PER_KV * SPAN, CHUNK * SPAN)
                peak = jnp.max(score, axis=1, keepdims=True)
                if not opening:
                    before = peaks[group]
                    peak = jnp.maximum(before, peak)
                weight = jnp.exp2(score - peak)
                total = jnp.sum(weight, axis=1, keepdims=True)
                update = jnp.dot(
                    weight.astype(jnp.bfloat16), value, preferred_element_type=jnp.float32
                )
                if not opening:
                    rescale = jnp.exp2(before - peak)
                    total = total + sums[group] * rescale
                    update = update + mixed[group] * rescale
                peaks[group] = peak
                sums[group] = total
                mixed[group] = update

        one_chunk(0, True)

        def later(chunk, carry):
            one_chunk(chunk, False)
            return carry

        lax.fori_loop(1, totals_listed[half], later, 0)
        for group in range(KEY_VALUE_HEADS):
            result = (mixed[group] * (1.0 / sums[group])).astype(jnp.bfloat16)
            for h in range(QUERIES_PER_KV):
                out_ref[
                    pl.ds(pl.multiple_of(half * SPAN, SPAN), SPAN),
                    pl.ds((group * QUERIES_PER_KV + h) * HEAD_SIZE, HEAD_SIZE),
                ] = result[h * SPAN : (h + 1) * SPAN]
        return unused

    lax.fori_loop(0, 2, one_half, 0)


def attention(where, dest, order, lengths, query_arrays, arrays, pieces):
    count = len(arrays)
    smem = pl.BlockSpec(memory_space=pltpu.SMEM)
    anywhere = pl.BlockSpec(memory_space=pl.ANY)
    rows = QUERIES_PER_KV * SPAN
    return pl.pallas_call(
        functools.partial(attention_kernel, pieces, count),
        out_shape=jax.ShapeDtypeStruct((2 * SPAN, QUERY_WIDTH), jnp.bfloat16),
        in_specs=[smem] * 4 + [anywhere] * (3 + count),
        out_specs=pl.BlockSpec(memory_space=pltpu.VMEM),
        scratch_shapes=[
            pltpu.VMEM((2, SPAN, QUERY_WIDTH), jnp.bfloat16),
            pltpu.VMEM((SPANS * SPAN, HALF_WIDTH), jnp.bfloat16),
            pltpu.VMEM((SPANS * SPAN, HALF_WIDTH), jnp.bfloat16),
            pltpu.SMEM((2, LIST), jnp.int32),
            pltpu.SMEM((2, LIST), jnp.int32),
            pltpu.SMEM((2,), jnp.int32),
            pltpu.SMEM((2, NDOC), jnp.int32),
            pltpu.VMEM((KEY_VALUE_HEADS, rows, 1), jnp.float32),
            pltpu.VMEM((KEY_VALUE_HEADS, rows, 1), jnp.float32),
            pltpu.VMEM((KEY_VALUE_HEADS, rows, HEAD_SIZE), jnp.float32),
            pltpu.SemaphoreType.DMA((2,)),
            pltpu.SemaphoreType.DMA((SPANS, 2)),
        ],
        compiler_params=pltpu.CompilerParams(vmem_limit_bytes=32 * 1024 * 1024),
        cost_estimate=pl.CostEstimate(
            flops=1_000_000_000, bytes_accessed=4_000_000, transcendentals=2_000_000
        ),
        name="attend",
    )(where, dest, order, lengths, *query_arrays, *arrays)


def swaps(count, first):
    pairs = [(i % count, (i + 1) % count) for i in range(first, first + count, 2)]
    return pairs + [(b, a) for a, b in pairs]


def on_device(qkv, dest, order, lengths):
    dp_count = lax.axis_size("dp")
    dp_index = lax.axis_index("dp")
    column = lax.axis_index("ctx_0")
    row = lax.axis_index("ctx_1")
    columns = lax.axis_size("ctx_0")
    odd = dp_index & 1
    even_partner = dp_index + 1 - 2 * odd
    odd_partner = (dp_index - 1 + 2 * odd + dp_count) % dp_count
    resident = qkv[0]
    kv = resident[:, QUERY_WIDTH:]

    def trade(array, first):
        return lax.ppermute(array, "dp", swaps(dp_count, first))

    kv_odd = trade(kv, 1)
    kv_even = trade(kv, 0)
    own_sources = lax.dynamic_slice_in_dim(dest[0], 2 * (2 * column + row), 2)
    row_from = jnp.repeat(own_sources, SPAN)[:, None]
    own = jnp.where(
        row_from == even_partner, kv_even, jnp.where(row_from == odd_partner, kv_odd, kv)
    )
    other = lax.ppermute(own, "ctx_1", swaps(2, 0)[:2])

    def across(array, first):
        return lax.ppermute(array, "ctx_0", swaps(columns, first))

    arrays = [own, other]
    pieces = [(0, 0, 0, 0, 0), (0, SPAN, 0, 0, 1), (1, 0, 0, 1, 0), (1, SPAN, 0, 1, 1)]
    for flip, stream in enumerate((own, other)):
        even, odd_side = stream, stream
        for step in range(1, 4):
            even, odd_side = across(odd_side, 0), across(even, 1)
            for way, array in ((step, even), (-step, odd_side)):
                arrays.append(array)
                for part in range(2):
                    pieces.append((len(arrays) - 1, part * SPAN, way, flip, part))
        far = (across(odd_side[:SPAN], 0), across(even[SPAN:], 1))
        for part, array in enumerate(far):
            arrays.append(array)
            pieces.append((len(arrays) - 1, 0, 4, flip, part))
    queries, other = lax.optimization_barrier((resident[:, :QUERY_WIDTH], other))
    query_odd = trade(queries, 1)
    query_even = trade(queries, 0)
    lane = jnp.arange(8, dtype=jnp.int32)
    where = jnp.where(
        lane == 0,
        dp_index,
        jnp.where(
            lane == 1,
            column,
            jnp.where(lane == 2, row, jnp.where(lane == 3, even_partner, odd_partner)),
        ),
    ).astype(jnp.int32)
    attended = attention(
        where, dest, order, lengths, (resident, query_even, query_odd), arrays, pieces
    )
    return attended[None]


def solution(mesh):
    finer = Mesh(mesh.devices.reshape(mesh.shape["dp"], 8, 2), ("dp", "ctx_0", "ctx_1"))
    placed = (P("dp", CTX, None), P("dp", None), P(), P())
    return jax.shard_map(
        on_device, mesh=finer, in_specs=placed, out_specs=P("dp", CTX, None), check_vma=False
    )
```

```python
import functools
import math

import jax
import jax.numpy as jnp
from jax import lax
from jax.experimental import pallas as pl
from jax.experimental.pallas import tpu as pltpu
from jax.sharding import Mesh
from jax.sharding import PartitionSpec as P

QUERY_HEADS = 32
KEY_VALUE_HEADS = 4
HEAD_SIZE = 128
NDOC = 8
SPAN = 64
QUERIES_PER_KV = 8
CTX = ("ctx_0", "ctx_1")
QUERY_WIDTH = QUERY_HEADS * HEAD_SIZE
HALF_WIDTH = KEY_VALUE_HEADS * HEAD_SIZE
SPANS = 32
CHUNK = 4
LIST = 40
FAR = 1 << 20
MASK_FLOOR = -1e30
EXP2_SCALE = math.log2(math.e) / math.sqrt(HEAD_SIZE)


def attention_kernel(pieces, count, *refs):
    where_ref, dest_ref, order_ref, lengths_ref = refs[:4]
    query_refs = refs[4:7]
    piece_refs = refs[7 : 7 + count]
    out_ref = refs[7 + count]
    (
        queries,
        keys,
        values,
        listed,
        bases,
        totals_listed,
        ends,
        peaks,
        sums,
        mixed,
        query_sems,
        piece_sems,
    ) = refs[8 + count :]
    rank, column, row = where_ref[0], where_ref[1], where_ref[2]
    sign = 1 - 2 * (column & 1)
    own_slot = 2 * (2 * column + row)
    even_partner = where_ref[3]
    odd_partner = where_ref[4]

    def query_copy(half, which):
        rows = pl.ds(half * SPAN, SPAN)
        return pltpu.make_async_copy(
            query_refs[which].at[rows, pl.ds(0, QUERY_WIDTH)],
            queries.at[half],
            query_sems.at[half],
        )

    sources, spans, firsts = [], [], []
    for half in range(2):
        source = dest_ref[0, own_slot + half]
        for which, partner in enumerate((rank, even_partner, odd_partner)):

            @pl.when(source == partner)
            def _(half=half, which=which):
                query_copy(half, which).start()

        span = order_ref[own_slot + half]
        end, first = jnp.int32(0), jnp.int32(0)
        for doc in range(NDOC):
            end = end + lengths_ref[source, doc]
            ends[half, doc] = end
            first = jnp.where(end <= span * SPAN, end, first)
        sources.append(source)
        spans.append(span)
        firsts.append(first)

    def piece_copies(index):
        ref, first_row = pieces[index][0], pieces[index][1]
        rows = pl.ds(first_row, SPAN)
        there = pl.ds(index * SPAN, SPAN)
        return (
            pltpu.make_async_copy(
                piece_refs[ref].at[rows, pl.ds(0, HALF_WIDTH)], keys.at[there], piece_sems.at[index, 0]
            ),
            pltpu.make_async_copy(
                piece_refs[ref].at[rows, pl.ds(HALF_WIDTH, HALF_WIDTH)],
                values.at[there],
                piece_sems.at[index, 1],
            ),
        )

    counts = [jnp.int32(0), jnp.int32(0)]
    wanted = []
    for index, (_, _, step, flip, part) in enumerate(pieces):
        there = (column + sign * step) & 7
        slot = 2 * (2 * there + (row ^ flip)) + part
        source, span = dest_ref[0, slot], order_ref[slot]
        either = None
        for half in range(2):
            need = (
                (source == sources[half])
                & (span <= spans[half])
                & (span * SPAN + SPAN > firsts[half])
            )

            @pl.when(need)
            def _(half=half, index=index, span=span, at=counts[half]):
                listed[half, at] = index
                bases[half, at] = span * SPAN

            counts[half] = counts[half] + need.astype(jnp.int32)
            either = need if either is None else either | need
        wanted.append(either)

        @pl.when(either)
        def _(index=index):
            for copy in piece_copies(index):
                copy.start()

    for half in range(2):
        totals_listed[half] = (counts[half] + CHUNK - 1) // CHUNK
        for extra in range(CHUNK - 1):
            listed[half, counts[half] + extra] = half
            bases[half, counts[half] + extra] = FAR
        query_copy(half, 0).wait()
    for index in range(SPANS):

        @pl.when(wanted[index])
        def _(index=index):
            for copy in piece_copies(index):
                copy.wait()

    lane = lax.broadcasted_iota(jnp.int32, (1, CHUNK * SPAN), 1)

    def one_half(half, unused):
        position = order_ref[own_slot + half] * SPAN + lax.broadcasted_iota(jnp.int32, (SPAN, 1), 0)
        start = jnp.zeros((SPAN, 1), jnp.int32)
        for doc in range(NDOC):
            end = ends[half, doc]
            start = jnp.where(position >= end, end, start)

        def one_chunk(chunk, opening):
            at = chunk * CHUNK
            key_position = lane & (SPAN - 1)
            base = jnp.full((1, CHUNK * SPAN), bases[half, at], jnp.int32)
            for j in range(1, CHUNK):
                base = jnp.where(lane >= j * SPAN, bases[half, at + j], base)
            key_position = key_position + base
            visible = (key_position <= position) & (key_position >= start)
            bias = jnp.where(visible, 0.0, MASK_FLOOR).astype(jnp.float32)
            firsts_of = [pl.multiple_of(listed[half, at + j] * SPAN, SPAN) for j in range(CHUNK)]
            for group in range(KEY_VALUE_HEADS):
                columns = slice(group * HEAD_SIZE, (group + 1) * HEAD_SIZE)
                key = jnp.concatenate([keys[pl.ds(f, SPAN), columns] for f in firsts_of], axis=0)
                value = jnp.concatenate([values[pl.ds(f, SPAN), columns] for f in firsts_of], axis=0)
                query = jnp.concatenate(
                    [
                        queries[half, :, pl.ds((group * QUERIES_PER_KV + h) * HEAD_SIZE, HEAD_SIZE)]
                        for h in range(QUERIES_PER_KV)
                    ],
                    axis=0,
                )
                score = lax.dot_general(
                    query, key, (((1,), (1,)), ((), ())), preferred_element_type=jnp.float32
                )
                score = score.reshape(QUERIES_PER_KV, SPAN, CHUNK * SPAN) * EXP2_SCALE + bias[None]
                score = score.reshape(QUERIES_PER_KV * SPAN, CHUNK * SPAN)
                peak = jnp.max(score, axis=1, keepdims=True)
                if not opening:
                    before = peaks[group]
                    peak = jnp.maximum(before, peak)
                weight = jnp.exp2(score - peak)
                total = jnp.sum(weight, axis=1, keepdims=True)
                update = jnp.dot(
                    weight.astype(jnp.bfloat16), value, preferred_element_type=jnp.float32
                )
                if not opening:
                    rescale = jnp.exp2(before - peak)
                    total = total + sums[group] * rescale
                    update = update + mixed[group] * rescale
                peaks[group] = peak
                sums[group] = total
                mixed[group] = update

        one_chunk(0, True)

        def later(chunk, carry):
            one_chunk(chunk, False)
            return carry

        lax.fori_loop(1, totals_listed[half], later, 0)
        for group in range(KEY_VALUE_HEADS):
            result = (mixed[group] * (1.0 / sums[group])).astype(jnp.bfloat16)
            for h in range(QUERIES_PER_KV):
                out_ref[
                    pl.ds(pl.multiple_of(half * SPAN, SPAN), SPAN),
                    pl.ds((group * QUERIES_PER_KV + h) * HEAD_SIZE, HEAD_SIZE),
                ] = result[h * SPAN : (h + 1) * SPAN]
        return unused

    lax.fori_loop(0, 2, one_half, 0)


def attention(where, dest, order, lengths, query_arrays, arrays, pieces):
    count = len(arrays)
    smem = pl.BlockSpec(memory_space=pltpu.SMEM)
    anywhere = pl.BlockSpec(memory_space=pl.ANY)
    rows = QUERIES_PER_KV * SPAN
    return pl.pallas_call(
        functools.partial(attention_kernel, pieces, count),
        out_shape=jax.ShapeDtypeStruct((2 * SPAN, QUERY_WIDTH), jnp.bfloat16),
        in_specs=[smem] * 4 + [anywhere] * (3 + count),
        out_specs=pl.BlockSpec(memory_space=pltpu.VMEM),
        scratch_shapes=[
            pltpu.VMEM((2, SPAN, QUERY_WIDTH), jnp.bfloat16),
            pltpu.VMEM((SPANS * SPAN, HALF_WIDTH), jnp.bfloat16),
            pltpu.VMEM((SPANS * SPAN, HALF_WIDTH), jnp.bfloat16),
            pltpu.SMEM((2, LIST), jnp.int32),
            pltpu.SMEM((2, LIST), jnp.int32),
            pltpu.SMEM((2,), jnp.int32),
            pltpu.SMEM((2, NDOC), jnp.int32),
            pltpu.VMEM((KEY_VALUE_HEADS, rows, 1), jnp.float32),
            pltpu.VMEM((KEY_VALUE_HEADS, rows, 1), jnp.float32),
            pltpu.VMEM((KEY_VALUE_HEADS, rows, HEAD_SIZE), jnp.float32),
            pltpu.SemaphoreType.DMA((2,)),
            pltpu.SemaphoreType.DMA((SPANS, 2)),
        ],
        compiler_params=pltpu.CompilerParams(),
        cost_estimate=pl.CostEstimate(
            flops=1_000_000_000, bytes_accessed=4_000_000, transcendentals=2_000_000
        ),
        name="attend",
    )(where, dest, order, lengths, *query_arrays, *arrays)


def swaps(count, first):
    pairs = [(i % count, (i + 1) % count) for i in range(first, first + count, 2)]
    return pairs + [(b, a) for a, b in pairs]


def on_device(qkv, dest, order, lengths):
    dp_count = lax.axis_size("dp")
    dp_index = lax.axis_index("dp")
    column = lax.axis_index("ctx_0")
    row = lax.axis_index("ctx_1")
    columns = lax.axis_size("ctx_0")
    odd = dp_index & 1
    even_partner = dp_index + 1 - 2 * odd
    odd_partner = (dp_index - 1 + 2 * odd + dp_count) % dp_count
    resident = qkv[0]
    kv = resident[:, QUERY_WIDTH:]

    def trade(array, first):
        return lax.ppermute(array, "dp", swaps(dp_count, first))

    kv_odd = trade(kv, 1)
    kv_even = trade(kv, 0)
    own_sources = lax.dynamic_slice_in_dim(dest[0], 2 * (2 * column + row), 2)
    row_from = jnp.repeat(own_sources, SPAN)[:, None]
    own = jnp.where(
        row_from == even_partner, kv_even, jnp.where(row_from == odd_partner, kv_odd, kv)
    )
    other = lax.ppermute(own, "ctx_1", [(0, 1), (1, 0)])

    def across(array, first):
        return lax.ppermute(array, "ctx_0", swaps(columns, first))

    arrays = [own, other]
    ways = [0, 0]
    last = []
    for stream in (own, other):
        even, odd_side = stream, stream
        for step in range(1, 4):
            even, odd_side = across(odd_side, 0), across(even, 1)
            arrays += [even, odd_side]
            ways += [step, -step]
        last.append((even, odd_side))
    arrays += [across(last[0][1], 0), across(last[1][0], 1)]
    ways += [4, 4]
    flips = [0, 1] + [0] * 6 + [1] * 6 + [0, 1]
    pieces = [
        (index, part * SPAN, ways[index], flips[index], part)
        for index in range(len(arrays))
        for part in range(2)
    ]
    queries, _ = lax.optimization_barrier((resident[:, :QUERY_WIDTH], arrays[4]))
    query_odd = trade(queries, 1)
    query_even = trade(queries, 0)
    lane = jnp.arange(8, dtype=jnp.int32)
    where = jnp.where(
        lane == 0,
        dp_index,
        jnp.where(
            lane == 1,
            column,
            jnp.where(lane == 2, row, jnp.where(lane == 3, even_partner, odd_partner)),
        ),
    ).astype(jnp.int32)
    attended = attention(
        where, dest, order, lengths, (resident, query_even, query_odd), arrays, pieces
    )
    return attended[None]


def solution(mesh):
    finer = Mesh(mesh.devices.reshape(mesh.shape["dp"], 8, 2), ("dp", "ctx_0", "ctx_1"))
    placed = (P("dp", CTX, None), P("dp", None), P(), P())
    return jax.shard_map(
        on_device, mesh=finer, in_specs=placed, out_specs=P("dp", CTX, None), check_vma=False
    )
```

```python
import functools
import math

import jax
import jax.numpy as jnp
from jax import lax
from jax.experimental import pallas as pl
from jax.experimental.pallas import tpu as pltpu
from jax.sharding import Mesh
from jax.sharding import PartitionSpec as P


QUERY_HEADS = 32
KEY_VALUE_HEADS = 4
HEAD_SIZE = 128
NDOC = 8
SPAN = 64
QUERIES_PER_KV = 8
CTX = ("ctx_0", "ctx_1")
QUERY_WIDTH = QUERY_HEADS * HEAD_SIZE
HALF_WIDTH = KEY_VALUE_HEADS * HEAD_SIZE
SPANS = 32
CHUNK = 4
MOST_CHUNKS = 5
LISTED, BASES, WANTED = 0, 40, 80
ENDS, WHICH, POSITION, CHUNKS = 112, 120, 121, 122
PLAN = 128
KEEP = pl.ANY
FAR = 1 << 20
MASK_FLOOR = -1e30
EXP2_SCALE = math.log2(math.e) / math.sqrt(HEAD_SIZE)


def piece_slot(where_ref, piece):
    _, _, step, flip, part = piece
    column, row = where_ref[1], where_ref[2]
    there = (column + (1 - 2 * (column & 1)) * step) & 7
    return 2 * (2 * there + (row ^ flip)) + part


def list_kernel(pieces, where_ref, dest_ref, order_ref, lengths_ref, plan_ref):
    own_slot = 2 * (2 * where_ref[1] + where_ref[2])
    sources, spans, firsts = [], [], []
    for half in range(2):
        source = dest_ref[0, own_slot + half]
        plan_ref[half, WHICH] = jnp.where(
            source == where_ref[3], 1, jnp.where(source == where_ref[4], 2, 0)
        )
        span = order_ref[own_slot + half]
        plan_ref[half, POSITION] = span * SPAN
        end, first = jnp.int32(0), jnp.int32(0)
        for doc in range(NDOC):
            end = end + lengths_ref[source, doc]
            plan_ref[half, ENDS + doc] = end
            first = jnp.where(end <= span * SPAN, end, first)
        sources.append(source)
        spans.append(span)
        firsts.append(first)
    counts = [jnp.int32(0), jnp.int32(0)]
    for index, piece in enumerate(pieces):
        slot = piece_slot(where_ref, piece)
        source, span = dest_ref[0, slot], order_ref[slot]
        for half in range(2):
            need = (
                (source == sources[half])
                & (span <= spans[half])
                & (span * SPAN + SPAN > firsts[half])
            )
            plan_ref[half, LISTED + counts[half]] = index
            plan_ref[half, BASES + counts[half]] = span * SPAN
            need = need.astype(jnp.int32)
            plan_ref[half, WANTED + index] = need
            counts[half] = counts[half] + need
    for half in range(2):
        plan_ref[half, CHUNKS] = (counts[half] + CHUNK - 1) // CHUNK
        for extra in range(CHUNK - 1):
            plan_ref[half, LISTED + counts[half] + extra] = half
            plan_ref[half, BASES + counts[half] + extra] = FAR


def attention_kernel(pieces, count, *refs):
    plan = refs[0]
    query_refs = refs[1:4]
    piece_refs = refs[4 : 4 + count]
    out_ref = refs[4 + count]
    (queries, keys, values, scores, peaks, sums, mixed, outs, query_sems, piece_sems, out_sems) = refs[
        5 + count :
    ]

    def query_copy(half, which):
        rows = pl.ds(half * SPAN, SPAN)
        return pltpu.make_async_copy(
            query_refs[which].at[rows, pl.ds(0, QUERY_WIDTH)],
            queries.at[half],
            query_sems.at[half],
        )

    def out_copy(half):
        return pltpu.make_async_copy(
            outs.at[half], out_ref.at[pl.ds(half * SPAN, SPAN)], out_sems.at[half]
        )

    def piece_copies(index):
        ref, first_row = pieces[index][0], pieces[index][1]
        rows = pl.ds(first_row, SPAN)
        there = pl.ds(index * SPAN, SPAN)
        return (
            pltpu.make_async_copy(
                piece_refs[ref].at[rows, pl.ds(0, HALF_WIDTH)], keys.at[there], piece_sems.at[index, 0]
            ),
            pltpu.make_async_copy(
                piece_refs[ref].at[rows, pl.ds(HALF_WIDTH, HALF_WIDTH)],
                values.at[there],
                piece_sems.at[index, 1],
            ),
        )

    for half in range(2):
        for which in range(3):

            @pl.when(plan[half, WHICH] == which)
            def _(half=half, which=which):
                query_copy(half, which).start()

    for index in range(SPANS):

        @pl.when(plan[0, WANTED + index] + plan[1, WANTED + index] > 0)
        def _(index=index):
            for copy in piece_copies(index):
                copy.start()

    for half in range(2):
        query_copy(half, 0).wait()
    for index in range(SPANS):

        @pl.when(plan[0, WANTED + index] + plan[1, WANTED + index] > 0)
        def _(index=index):
            for copy in piece_copies(index):
                copy.wait()

    lane = lax.broadcasted_iota(jnp.int32, (1, CHUNK * SPAN), 1)
    rows = QUERIES_PER_KV * SPAN

    def one_half(half, unused):
        position = plan[half, POSITION] + lax.broadcasted_iota(jnp.int32, (SPAN, 1), 0)
        start = jnp.zeros((SPAN, 1), jnp.int32)
        for doc in range(NDOC):
            end = plan[half, ENDS + doc]
            start = jnp.where(position >= end, end, start)
        chunks = plan[half, CHUNKS]
        peaks[...] = jnp.full_like(peaks, MASK_FLOOR)
        sums[...] = jnp.zeros_like(sums)
        mixed[...] = jnp.zeros_like(mixed)

        def first_rows(chunk):
            return [
                pl.multiple_of(plan[half, LISTED + chunk * CHUNK + j] * SPAN, SPAN)
                for j in range(CHUNK)
            ]

        def score_chunk(chunk, carry):
            at = BASES + chunk * CHUNK
            base = jnp.full((1, CHUNK * SPAN), plan[half, at], jnp.int32)
            for j in range(1, CHUNK):
                base = jnp.where(lane >= j * SPAN, plan[half, at + j], base)
            key_position = (lane & (SPAN - 1)) + base
            visible = (key_position <= position) & (key_position >= start)
            bias = jnp.where(visible, 0.0, MASK_FLOOR).astype(jnp.float32)
            firsts_of = first_rows(chunk)
            for group in range(KEY_VALUE_HEADS):
                columns = slice(group * HEAD_SIZE, (group + 1) * HEAD_SIZE)
                key = jnp.concatenate([keys[pl.ds(f, SPAN), columns] for f in firsts_of], axis=0)
                query = jnp.concatenate(
                    [
                        queries[half, :, pl.ds((group * QUERIES_PER_KV + h) * HEAD_SIZE, HEAD_SIZE)]
                        for h in range(QUERIES_PER_KV)
                    ],
                    axis=0,
                )
                score = lax.dot_general(
                    query, key, (((1,), (1,)), ((), ())), preferred_element_type=jnp.float32
                )
                score = score.reshape(QUERIES_PER_KV, SPAN, CHUNK * SPAN) * EXP2_SCALE + bias[None]
                score = score.reshape(rows, CHUNK * SPAN)
                scores[chunk, group] = score
                peak = peaks[group]
                for j in range(0, CHUNK * SPAN, HEAD_SIZE):
                    peak = jnp.maximum(peak, score[:, j : j + HEAD_SIZE])
                peaks[group] = peak
            return carry

        lax.fori_loop(0, chunks, score_chunk, 0)
        for group in range(KEY_VALUE_HEADS):
            peaks[group] = jnp.broadcast_to(
                jnp.max(peaks[group], axis=1, keepdims=True), (rows, HEAD_SIZE)
            )

        def mix_chunk(chunk, carry):
            firsts_of = first_rows(chunk)
            for group in range(KEY_VALUE_HEADS):
                columns = slice(group * HEAD_SIZE, (group + 1) * HEAD_SIZE)
                value = jnp.concatenate([values[pl.ds(f, SPAN), columns] for f in firsts_of], axis=0)
                peak = peaks[group]
                total = sums[group]
                weights = []
                for j in range(0, CHUNK * SPAN, HEAD_SIZE):
                    weight = jnp.exp2(scores[chunk, group, :, j : j + HEAD_SIZE] - peak)
                    total = total + weight
                    weights.append(weight.astype(jnp.bfloat16))
                sums[group] = total
                mixed[group] += jnp.dot(
                    jnp.concatenate(weights, axis=1), value, preferred_element_type=jnp.float32
                )
            return carry

        lax.fori_loop(0, chunks, mix_chunk, 0)
        for group in range(KEY_VALUE_HEADS):
            total = jnp.sum(sums[group], axis=1, keepdims=True)
            result = (mixed[group] * (1.0 / total)).astype(jnp.bfloat16)
            for h in range(QUERIES_PER_KV):
                outs[half, :, pl.ds((group * QUERIES_PER_KV + h) * HEAD_SIZE, HEAD_SIZE)] = result[
                    h * SPAN : (h + 1) * SPAN
                ]
        out_copy(half).start()
        return unused

    lax.fori_loop(0, 2, one_half, 0)
    for half in range(2):
        out_copy(half).wait()


def list_key_spans(where, dest, order, lengths, pieces):
    smem = pl.BlockSpec(memory_space=pltpu.SMEM)
    return pl.pallas_call(
        functools.partial(list_kernel, pieces),
        out_shape=jax.ShapeDtypeStruct((2, PLAN), jnp.int32),
        in_specs=[smem] * 4,
        out_specs=smem,
        cost_estimate=pl.CostEstimate(flops=4_000_000, bytes_accessed=4_000, transcendentals=0),
        name="list_spans",
    )(where, dest, order, lengths)


def attention(plan, query_arrays, arrays, pieces):
    count = len(arrays)
    smem = pl.BlockSpec(memory_space=pltpu.SMEM)
    anywhere = pl.BlockSpec(memory_space=KEEP)
    rows = QUERIES_PER_KV * SPAN
    return pl.pallas_call(
        functools.partial(attention_kernel, pieces, count),
        out_shape=jax.ShapeDtypeStruct((2 * SPAN, QUERY_WIDTH), jnp.bfloat16),
        in_specs=[smem] + [anywhere] * (3 + count),
        out_specs=pl.BlockSpec(memory_space=KEEP),
        scratch_shapes=[
            pltpu.VMEM((2, SPAN, QUERY_WIDTH), jnp.bfloat16),
            pltpu.VMEM((SPANS * SPAN, HALF_WIDTH), jnp.bfloat16),
            pltpu.VMEM((SPANS * SPAN, HALF_WIDTH), jnp.bfloat16),
            pltpu.VMEM((MOST_CHUNKS, KEY_VALUE_HEADS, rows, CHUNK * SPAN), jnp.float32),
            pltpu.VMEM((KEY_VALUE_HEADS, rows, HEAD_SIZE), jnp.float32),
            pltpu.VMEM((KEY_VALUE_HEADS, rows, HEAD_SIZE), jnp.float32),
            pltpu.VMEM((KEY_VALUE_HEADS, rows, HEAD_SIZE), jnp.float32),
            pltpu.VMEM((2, SPAN, QUERY_WIDTH), jnp.bfloat16),
            pltpu.SemaphoreType.DMA((2,)),
            pltpu.SemaphoreType.DMA((SPANS, 2)),
            pltpu.SemaphoreType.DMA((2,)),
        ],
        cost_estimate=pl.CostEstimate(
            flops=1_000_000_000, bytes_accessed=4_000_000, transcendentals=2_000_000
        ),
        name="attend",
    )(plan, *query_arrays, *arrays)


def swaps(count, first):
    pairs = [(i % count, (i + 1) % count) for i in range(first, first + count, 2)]
    return pairs + [(b, a) for a, b in pairs]


def on_device(qkv, dest, order, lengths):
    dp_count = lax.axis_size("dp")
    dp_index = lax.axis_index("dp")
    column = lax.axis_index("ctx_0")
    row = lax.axis_index("ctx_1")
    columns = lax.axis_size("ctx_0")
    odd = dp_index & 1
    even_partner = dp_index + 1 - 2 * odd
    odd_partner = (dp_index - 1 + 2 * odd + dp_count) % dp_count
    resident = qkv[0]

    def trade(array, first):
        return lax.ppermute(array, "dp", swaps(dp_count, first))

    kv = resident[:, QUERY_WIDTH:]
    query_odd = trade(resident, 1)
    even_rows = trade(resident, 0)
    kv_odd = trade(kv, 1)
    kv_even = even_rows[:, QUERY_WIDTH:]
    own_sources = lax.dynamic_slice_in_dim(dest[0], 2 * (2 * column + row), 2)
    row_from = jnp.repeat(own_sources, SPAN)[:, None]
    own = jnp.where(
        row_from == even_partner, kv_even, jnp.where(row_from == odd_partner, kv_odd, kv)
    )
    other = lax.ppermute(own, "ctx_1", [(0, 1), (1, 0)])

    def across(array, first):
        return lax.ppermute(array, "ctx_0", swaps(columns, first))

    arrays = [own, other]
    ways = [0, 0]
    last = []
    for stream in (own, other):
        even, odd_side = stream, stream
        for step in range(1, 4):
            even, odd_side = across(odd_side, 0), across(even, 1)
            arrays += [even, odd_side]
            ways += [step, -step]
        last.append((even, odd_side))
    arrays += [across(last[0][1], 0), across(last[1][0], 1)]
    ways += [4, 4]
    flips = [0, 1] + [0] * 6 + [1] * 6 + [0, 1]
    pieces = [
        (index, part * SPAN, ways[index], flips[index], part)
        for index in range(len(arrays))
        for part in range(2)
    ]
    lane = jnp.arange(8, dtype=jnp.int32)
    where = jnp.where(
        lane == 0,
        dp_index,
        jnp.where(
            lane == 1,
            column,
            jnp.where(lane == 2, row, jnp.where(lane == 3, even_partner, odd_partner)),
        ),
    ).astype(jnp.int32)
    plan = list_key_spans(where, dest, order, lengths, pieces)
    attended = attention(plan, (resident, even_rows, query_odd), arrays, pieces)
    return attended[None]


def solution(mesh):
    finer = Mesh(mesh.devices.reshape(mesh.shape["dp"], 8, 2), ("dp", "ctx_0", "ctx_1"))
    placed = (P("dp", CTX, None), P("dp", None), P(), P())

    return jax.shard_map(
        on_device, mesh=finer, in_specs=placed, out_specs=P("dp", CTX, None), check_vma=False
    )
```

```python
import functools
import math

import jax
import jax.numpy as jnp
from jax import lax
from jax.experimental import pallas as pl
from jax.experimental.pallas import tpu as pltpu
from jax.sharding import Mesh
from jax.sharding import PartitionSpec as P


QUERY_HEADS = 32
KEY_VALUE_HEADS = 4
HEAD_SIZE = 128
NDOC = 8
SPAN = 64
QUERIES_PER_KV = 8
CTX = ("ctx_0", "ctx_1")
QUERY_WIDTH = QUERY_HEADS * HEAD_SIZE
HALF_WIDTH = KEY_VALUE_HEADS * HEAD_SIZE
SPANS = 32
CHUNK = 4
MOST_CHUNKS = 5
LISTED, BASES, WANTED = 0, 40, 80
ENDS, WHICH, POSITION, CHUNKS = 112, 120, 121, 122
PLAN = 128
KEEP = pl.ANY
FAR = 1 << 20
MASK_FLOOR = -1e30
EXP2_SCALE = math.log2(math.e) / math.sqrt(HEAD_SIZE)


def piece_slot(where_ref, piece):
    _, _, step, flip, part = piece
    column, row = where_ref[1], where_ref[2]
    there = (column + (1 - 2 * (column & 1)) * step) & 7
    return 2 * (2 * there + (row ^ flip)) + part


def list_kernel(pieces, where_ref, dest_ref, order_ref, lengths_ref, plan_ref):
    own_slot = 2 * (2 * where_ref[1] + where_ref[2])
    sources, spans, firsts = [], [], []
    for half in range(2):
        source = dest_ref[0, own_slot + half]
        plan_ref[half, WHICH] = jnp.where(
            source == where_ref[3], 1, jnp.where(source == where_ref[4], 2, 0)
        )
        span = order_ref[own_slot + half]
        plan_ref[half, POSITION] = span * SPAN
        end, first = jnp.int32(0), jnp.int32(0)
        for doc in range(NDOC):
            end = end + lengths_ref[source, doc]
            plan_ref[half, ENDS + doc] = end
            first = jnp.where(end <= span * SPAN, end, first)
        sources.append(source)
        spans.append(span)
        firsts.append(first)
    counts = [jnp.int32(0), jnp.int32(0)]
    for index, piece in enumerate(pieces):
        slot = piece_slot(where_ref, piece)
        source, span = dest_ref[0, slot], order_ref[slot]
        for half in range(2):
            need = (
                (source == sources[half])
                & (span <= spans[half])
                & (span * SPAN + SPAN > firsts[half])
            )
            plan_ref[half, LISTED + counts[half]] = index
            plan_ref[half, BASES + counts[half]] = span * SPAN
            need = need.astype(jnp.int32)
            plan_ref[half, WANTED + index] = need
            counts[half] = counts[half] + need
    for half in range(2):
        plan_ref[half, CHUNKS] = (counts[half] + CHUNK - 1) // CHUNK
        for extra in range(CHUNK - 1):
            plan_ref[half, LISTED + counts[half] + extra] = half
            plan_ref[half, BASES + counts[half] + extra] = FAR


def attention_kernel(pieces, count, *refs):
    plan = refs[0]
    query_refs = refs[1:4]
    piece_refs = refs[4 : 4 + count]
    out_ref = refs[4 + count]
    (queries, keys, values, scores, peaks, sums, mixed, outs, query_sems, piece_sems, out_sems) = refs[
        5 + count :
    ]

    def query_copy(half, which):
        rows = pl.ds(half * SPAN, SPAN)
        return pltpu.make_async_copy(
            query_refs[which].at[rows, pl.ds(0, QUERY_WIDTH)],
            queries.at[half],
            query_sems.at[half],
        )

    def out_copy(half):
        return pltpu.make_async_copy(
            outs.at[half], out_ref.at[pl.ds(half * SPAN, SPAN)], out_sems.at[half]
        )

    def piece_copies(index):
        ref, first_row = pieces[index][0], pieces[index][1]
        rows = pl.ds(first_row, SPAN)
        there = pl.ds(index * SPAN, SPAN)
        return (
            pltpu.make_async_copy(
                piece_refs[ref].at[rows, pl.ds(0, HALF_WIDTH)], keys.at[there], piece_sems.at[index, 0]
            ),
            pltpu.make_async_copy(
                piece_refs[ref].at[rows, pl.ds(HALF_WIDTH, HALF_WIDTH)],
                values.at[there],
                piece_sems.at[index, 1],
            ),
        )

    for half in range(2):
        for which in range(3):

            @pl.when(plan[half, WHICH] == which)
            def _(half=half, which=which):
                query_copy(half, which).start()

    for index in range(SPANS):

        @pl.when(plan[0, WANTED + index] + plan[1, WANTED + index] > 0)
        def _(index=index):
            for copy in piece_copies(index):
                copy.start()

    for half in range(2):
        query_copy(half, 0).wait()
    for index in range(SPANS):

        @pl.when(plan[0, WANTED + index] + plan[1, WANTED + index] > 0)
        def _(index=index):
            for copy in piece_copies(index):
                copy.wait()

    lane = lax.broadcasted_iota(jnp.int32, (1, CHUNK * SPAN), 1)
    rows = QUERIES_PER_KV * SPAN

    def one_half(half, unused):
        position = plan[half, POSITION] + lax.broadcasted_iota(jnp.int32, (SPAN, 1), 0)
        start = jnp.zeros((SPAN, 1), jnp.int32)
        for doc in range(NDOC):
            end = plan[half, ENDS + doc]
            start = jnp.where(position >= end, end, start)
        chunks = plan[half, CHUNKS]
        peaks[...] = jnp.full_like(peaks, MASK_FLOOR)
        sums[...] = jnp.zeros_like(sums)
        mixed[...] = jnp.zeros_like(mixed)

        def first_rows(chunk):
            return [
                pl.multiple_of(plan[half, LISTED + chunk * CHUNK + j] * SPAN, SPAN)
                for j in range(CHUNK)
            ]

        def score_chunk(chunk, carry):
            at = BASES + chunk * CHUNK
            base = jnp.full((1, CHUNK * SPAN), plan[half, at], jnp.int32)
            for j in range(1, CHUNK):
                base = jnp.where(lane >= j * SPAN, plan[half, at + j], base)
            key_position = (lane & (SPAN - 1)) + base
            visible = (key_position <= position) & (key_position >= start)
            bias = jnp.where(visible, 0.0, MASK_FLOOR).astype(jnp.float32)
            firsts_of = first_rows(chunk)
            for group in range(KEY_VALUE_HEADS):
                columns = slice(group * HEAD_SIZE, (group + 1) * HEAD_SIZE)
                key = jnp.concatenate([keys[pl.ds(f, SPAN), columns] for f in firsts_of], axis=0)
                query = jnp.concatenate(
                    [
                        queries[half, :, pl.ds((group * QUERIES_PER_KV + h) * HEAD_SIZE, HEAD_SIZE)]
                        for h in range(QUERIES_PER_KV)
                    ],
                    axis=0,
                )
                score = lax.dot_general(
                    query, key, (((1,), (1,)), ((), ())), preferred_element_type=jnp.float32
                )
                score = score.reshape(QUERIES_PER_KV, SPAN, CHUNK * SPAN) * EXP2_SCALE + bias[None]
                score = score.reshape(rows, CHUNK * SPAN)
                scores[chunk, group] = score
                peak = peaks[group]
                for j in range(0, CHUNK * SPAN, HEAD_SIZE):
                    peak = jnp.maximum(peak, score[:, j : j + HEAD_SIZE])
                peaks[group] = peak
            return carry

        lax.fori_loop(0, chunks, score_chunk, 0)
        for group in range(KEY_VALUE_HEADS):
            peaks[group] = jnp.broadcast_to(
                jnp.max(peaks[group], axis=1, keepdims=True), (rows, HEAD_SIZE)
            )

        def mix_chunk(chunk, carry):
            firsts_of = first_rows(chunk)
            for group in range(KEY_VALUE_HEADS):
                columns = slice(group * HEAD_SIZE, (group + 1) * HEAD_SIZE)
                value = jnp.concatenate([values[pl.ds(f, SPAN), columns] for f in firsts_of], axis=0)
                peak = peaks[group]
                total = sums[group]
                weights = []
                for j in range(0, CHUNK * SPAN, HEAD_SIZE):
                    weight = jnp.exp2(scores[chunk, group, :, j : j + HEAD_SIZE] - peak)
                    total = total + weight
                    weights.append(weight.astype(jnp.bfloat16))
                sums[group] = total
                mixed[group] += jnp.dot(
                    jnp.concatenate(weights, axis=1), value, preferred_element_type=jnp.float32
                )
            return carry

        lax.fori_loop(0, chunks, mix_chunk, 0)
        for group in range(KEY_VALUE_HEADS):
            total = jnp.sum(sums[group], axis=1, keepdims=True)
            result = (mixed[group] * (1.0 / total)).astype(jnp.bfloat16)
            for h in range(QUERIES_PER_KV):
                outs[half, :, pl.ds((group * QUERIES_PER_KV + h) * HEAD_SIZE, HEAD_SIZE)] = result[
                    h * SPAN : (h + 1) * SPAN
                ]
        out_copy(half).start()
        return unused

    lax.fori_loop(0, 2, one_half, 0)
    for half in range(2):
        out_copy(half).wait()


def list_key_spans(where, dest, order, lengths, pieces):
    smem = pl.BlockSpec(memory_space=pltpu.SMEM)
    return pl.pallas_call(
        functools.partial(list_kernel, pieces),
        out_shape=jax.ShapeDtypeStruct((2, PLAN), jnp.int32),
        in_specs=[smem] * 4,
        out_specs=smem,
        cost_estimate=pl.CostEstimate(flops=4_000_000, bytes_accessed=4_000, transcendentals=0),
        name="list_spans",
    )(where, dest, order, lengths)


def attention(plan, query_arrays, arrays, pieces):
    count = len(arrays)
    smem = pl.BlockSpec(memory_space=pltpu.SMEM)
    anywhere = pl.BlockSpec(memory_space=KEEP)
    rows = QUERIES_PER_KV * SPAN
    return pl.pallas_call(
        functools.partial(attention_kernel, pieces, count),
        out_shape=jax.ShapeDtypeStruct((2 * SPAN, QUERY_WIDTH), jnp.bfloat16),
        in_specs=[smem] + [anywhere] * (3 + count),
        out_specs=pl.BlockSpec(memory_space=KEEP),
        scratch_shapes=[
            pltpu.VMEM((2, SPAN, QUERY_WIDTH), jnp.bfloat16),
            pltpu.VMEM((SPANS * SPAN, HALF_WIDTH), jnp.bfloat16),
            pltpu.VMEM((SPANS * SPAN, HALF_WIDTH), jnp.bfloat16),
            pltpu.VMEM((MOST_CHUNKS, KEY_VALUE_HEADS, rows, CHUNK * SPAN), jnp.float32),
            pltpu.VMEM((KEY_VALUE_HEADS, rows, HEAD_SIZE), jnp.float32),
            pltpu.VMEM((KEY_VALUE_HEADS, rows, HEAD_SIZE), jnp.float32),
            pltpu.VMEM((KEY_VALUE_HEADS, rows, HEAD_SIZE), jnp.float32),
            pltpu.VMEM((2, SPAN, QUERY_WIDTH), jnp.bfloat16),
            pltpu.SemaphoreType.DMA((2,)),
            pltpu.SemaphoreType.DMA((SPANS, 2)),
            pltpu.SemaphoreType.DMA((2,)),
        ],
        cost_estimate=pl.CostEstimate(
            flops=1_000_000_000, bytes_accessed=4_000_000, transcendentals=2_000_000
        ),
        name="attend",
    )(plan, *query_arrays, *arrays)


def swaps(count, first):
    pairs = [(i % count, (i + 1) % count) for i in range(first, first + count, 2)]
    return pairs + [(b, a) for a, b in pairs]


def on_device(qkv, dest, order, lengths):
    dp_count = lax.axis_size("dp")
    dp_index = lax.axis_index("dp")
    column = lax.axis_index("ctx_0")
    row = lax.axis_index("ctx_1")
    columns = lax.axis_size("ctx_0")
    odd = dp_index & 1
    even_partner = dp_index + 1 - 2 * odd
    odd_partner = (dp_index - 1 + 2 * odd + dp_count) % dp_count
    resident = qkv[0]

    def trade(array, first):
        return lax.ppermute(array, "dp", swaps(dp_count, first))

    kv = resident[:, QUERY_WIDTH:]
    kv_across = lax.ppermute(kv, "ctx_1", [(0, 1), (1, 0)])
    query_odd = trade(resident, 1)
    other_even = trade(kv_across, 0)
    even_rows = trade(resident, 0)
    other_odd = trade(kv_across, 1)
    kv_odd = trade(kv, 1)

    def settled(at_row, kept, from_even, from_odd):
        sources = lax.dynamic_slice_in_dim(dest[0], 2 * (2 * column + at_row), 2)
        row_from = jnp.repeat(sources, SPAN)[:, None]
        return jnp.where(
            row_from == even_partner, from_even, jnp.where(row_from == odd_partner, from_odd, kept)
        )

    own = settled(row, kv, even_rows[:, QUERY_WIDTH:], kv_odd)
    other = settled(1 - row, kv_across, other_even, other_odd)

    def across(array, first):
        return lax.ppermute(array, "ctx_0", swaps(columns, first))

    arrays = [own, other]
    ways = [0, 0]
    last = []
    for stream in (own, other):
        even, odd_side = stream, stream
        for step in range(1, 4):
            even, odd_side = across(odd_side, 0), across(even, 1)
            arrays += [even, odd_side]
            ways += [step, -step]
        last.append((even, odd_side))
    arrays += [across(last[0][1], 0), across(last[1][0], 1)]
    ways += [4, 4]
    flips = [0, 1] + [0] * 6 + [1] * 6 + [0, 1]
    pieces = [
        (index, part * SPAN, ways[index], flips[index], part)
        for index in range(len(arrays))
        for part in range(2)
    ]
    lane = jnp.arange(8, dtype=jnp.int32)
    where = jnp.where(
        lane == 0,
        dp_index,
        jnp.where(
            lane == 1,
            column,
            jnp.where(lane == 2, row, jnp.where(lane == 3, even_partner, odd_partner)),
        ),
    ).astype(jnp.int32)
    plan = list_key_spans(where, dest, order, lengths, pieces)
    attended = attention(plan, (resident, even_rows, query_odd), arrays, pieces)
    return attended[None]


def solution(mesh):
    finer = Mesh(mesh.devices.reshape(mesh.shape["dp"], 8, 2), ("dp", "ctx_0", "ctx_1"))
    placed = (P("dp", CTX, None), P("dp", None), P(), P())

    return jax.shard_map(
        on_device, mesh=finer, in_specs=placed, out_specs=P("dp", CTX, None), check_vma=False
    )
```

```python
import functools
import math

import jax
import jax.numpy as jnp
from jax import lax
from jax.experimental import pallas as pl
from jax.experimental.pallas import tpu as pltpu
from jax.sharding import Mesh
from jax.sharding import PartitionSpec as P


QUERY_HEADS = 32
KEY_VALUE_HEADS = 4
HEAD_SIZE = 128
NDOC = 8
SPAN = 64
QUERIES_PER_KV = 8
CTX = ("ctx_0", "ctx_1")
QUERY_WIDTH = QUERY_HEADS * HEAD_SIZE
HALF_WIDTH = KEY_VALUE_HEADS * HEAD_SIZE
SPANS = 32
CHUNK = 4
MOST_CHUNKS = 5
LISTED, BASES, WANTED = 0, 40, 80
ENDS, WHICH, POSITION, CHUNKS = 112, 120, 121, 122
PLAN = 128
KEEP = pl.ANY
FAR = 1 << 20
MASK_FLOOR = -1e30
EXP2_SCALE = math.log2(math.e) / math.sqrt(HEAD_SIZE)


def piece_slot(where_ref, piece):
    _, _, step, flip, part = piece
    column, row = where_ref[1], where_ref[2]
    there = (column + (1 - 2 * (column & 1)) * step) & 7
    return 2 * (2 * there + (row ^ flip)) + part


def list_kernel(pieces, where_ref, dest_ref, order_ref, lengths_ref, plan_ref):
    own_slot = 2 * (2 * where_ref[1] + where_ref[2])
    sources, spans, firsts = [], [], []
    for half in range(2):
        source = dest_ref[0, own_slot + half]
        plan_ref[half, WHICH] = jnp.where(
            source == where_ref[3], 1, jnp.where(source == where_ref[4], 2, 0)
        )
        span = order_ref[own_slot + half]
        plan_ref[half, POSITION] = span * SPAN
        end, first = jnp.int32(0), jnp.int32(0)
        for doc in range(NDOC):
            end = end + lengths_ref[source, doc]
            plan_ref[half, ENDS + doc] = end
            first = jnp.where(end <= span * SPAN, end, first)
        sources.append(source)
        spans.append(span)
        firsts.append(first)
    counts = [jnp.int32(0), jnp.int32(0)]
    for index, piece in enumerate(pieces):
        slot = piece_slot(where_ref, piece)
        source, span = dest_ref[0, slot], order_ref[slot]
        for half in range(2):
            need = (
                (source == sources[half])
                & (span <= spans[half])
                & (span * SPAN + SPAN > firsts[half])
            )
            plan_ref[half, LISTED + counts[half]] = index
            plan_ref[half, BASES + counts[half]] = span * SPAN
            need = need.astype(jnp.int32)
            plan_ref[half, WANTED + index] = need
            counts[half] = counts[half] + need
    for half in range(2):
        plan_ref[half, CHUNKS] = (counts[half] + CHUNK - 1) // CHUNK
        for extra in range(CHUNK - 1):
            plan_ref[half, LISTED + counts[half] + extra] = half
            plan_ref[half, BASES + counts[half] + extra] = FAR


def attention_kernel(pieces, count, *refs):
    plan = refs[0]
    query_refs = refs[1:4]
    piece_refs = refs[4 : 4 + count]
    out_ref = refs[4 + count]
    (queries, keys, values, scores, peaks, sums, mixed, outs, query_sems, piece_sems, out_sems) = refs[
        5 + count :
    ]

    def query_copy(half, which):
        rows = pl.ds(half * SPAN, SPAN)
        return pltpu.make_async_copy(
            query_refs[which].at[rows, pl.ds(0, QUERY_WIDTH)],
            queries.at[half],
            query_sems.at[half],
        )

    def out_copy(half):
        return pltpu.make_async_copy(
            outs.at[half], out_ref.at[pl.ds(half * SPAN, SPAN)], out_sems.at[half]
        )

    def piece_copies(index):
        ref, first_row = pieces[index][0], pieces[index][1]
        rows = pl.ds(first_row, SPAN)
        there = pl.ds(index * SPAN, SPAN)
        return (
            pltpu.make_async_copy(
                piece_refs[ref].at[rows, pl.ds(0, HALF_WIDTH)], keys.at[there], piece_sems.at[index, 0]
            ),
            pltpu.make_async_copy(
                piece_refs[ref].at[rows, pl.ds(HALF_WIDTH, HALF_WIDTH)],
                values.at[there],
                piece_sems.at[index, 1],
            ),
        )

    def for_wanted(act):
        for index in range(SPANS):

            @pl.when(plan[0, WANTED + index] + plan[1, WANTED + index] > 0)
            def _(index=index):
                act(piece_copies(index))

    for half in range(2):
        for which in range(3):

            @pl.when(plan[half, WHICH] == which)
            def _(half=half, which=which):
                query_copy(half, which).start()

        for_wanted(lambda copies: copies[half].start())

    for_wanted(lambda copies: copies[0].wait())
    lane = lax.broadcasted_iota(jnp.int32, (1, CHUNK * SPAN), 1)
    rows = QUERIES_PER_KV * SPAN

    def one_half(half, unused):
        position = plan[half, POSITION] + lax.broadcasted_iota(jnp.int32, (SPAN, 1), 0)
        start = jnp.zeros((SPAN, 1), jnp.int32)
        for doc in range(NDOC):
            end = plan[half, ENDS + doc]
            start = jnp.where(position >= end, end, start)
        chunks = plan[half, CHUNKS]
        query_copy(half, 0).wait()
        peaks[...] = jnp.full_like(peaks, MASK_FLOOR)
        sums[...] = jnp.zeros_like(sums)
        mixed[...] = jnp.zeros_like(mixed)

        def first_rows(chunk):
            return [
                pl.multiple_of(plan[half, LISTED + chunk * CHUNK + j] * SPAN, SPAN)
                for j in range(CHUNK)
            ]

        def score_chunk(chunk, carry):
            at = BASES + chunk * CHUNK
            base = jnp.full((1, CHUNK * SPAN), plan[half, at], jnp.int32)
            for j in range(1, CHUNK):
                base = jnp.where(lane >= j * SPAN, plan[half, at + j], base)
            key_position = (lane & (SPAN - 1)) + base
            visible = (key_position <= position) & (key_position >= start)
            bias = jnp.where(visible, 0.0, MASK_FLOOR).astype(jnp.float32)
            firsts_of = first_rows(chunk)
            for group in range(KEY_VALUE_HEADS):
                columns = slice(group * HEAD_SIZE, (group + 1) * HEAD_SIZE)
                key = jnp.concatenate([keys[pl.ds(f, SPAN), columns] for f in firsts_of], axis=0)
                query = jnp.concatenate(
                    [
                        queries[half, :, pl.ds((group * QUERIES_PER_KV + h) * HEAD_SIZE, HEAD_SIZE)]
                        for h in range(QUERIES_PER_KV)
                    ],
                    axis=0,
                )
                score = lax.dot_general(
                    query, key, (((1,), (1,)), ((), ())), preferred_element_type=jnp.float32
                )
                score = score.reshape(QUERIES_PER_KV, SPAN, CHUNK * SPAN) * EXP2_SCALE + bias[None]
                score = score.reshape(rows, CHUNK * SPAN)
                scores[chunk, group] = score
                peak = peaks[group]
                for j in range(0, CHUNK * SPAN, HEAD_SIZE):
                    peak = jnp.maximum(peak, score[:, j : j + HEAD_SIZE])
                peaks[group] = peak
            return carry

        lax.fori_loop(0, chunks, score_chunk, 0)
        for group in range(KEY_VALUE_HEADS):
            peaks[group] = jnp.broadcast_to(
                jnp.max(peaks[group], axis=1, keepdims=True), (rows, HEAD_SIZE)
            )

        @pl.when(half == 0)
        def _():
            for_wanted(lambda copies: copies[1].wait())

        def mix_chunk(chunk, carry):
            firsts_of = first_rows(chunk)
            for group in range(KEY_VALUE_HEADS):
                columns = slice(group * HEAD_SIZE, (group + 1) * HEAD_SIZE)
                value = jnp.concatenate([values[pl.ds(f, SPAN), columns] for f in firsts_of], axis=0)
                peak = peaks[group]
                total = sums[group]
                weights = []
                for j in range(0, CHUNK * SPAN, HEAD_SIZE):
                    weight = jnp.exp2(scores[chunk, group, :, j : j + HEAD_SIZE] - peak)
                    total = total + weight
                    weights.append(weight.astype(jnp.bfloat16))
                sums[group] = total
                mixed[group] += jnp.dot(
                    jnp.concatenate(weights, axis=1), value, preferred_element_type=jnp.float32
                )
            return carry

        lax.fori_loop(0, chunks, mix_chunk, 0)
        for group in range(KEY_VALUE_HEADS):
            total = jnp.sum(sums[group], axis=1, keepdims=True)
            result = (mixed[group] * (1.0 / total)).astype(jnp.bfloat16)
            for h in range(QUERIES_PER_KV):
                outs[half, :, pl.ds((group * QUERIES_PER_KV + h) * HEAD_SIZE, HEAD_SIZE)] = result[
                    h * SPAN : (h + 1) * SPAN
                ]
        out_copy(half).start()
        return unused

    lax.fori_loop(0, 2, one_half, 0)
    for half in range(2):
        out_copy(half).wait()


def list_key_spans(where, dest, order, lengths, pieces):
    smem = pl.BlockSpec(memory_space=pltpu.SMEM)
    return pl.pallas_call(
        functools.partial(list_kernel, pieces),
        out_shape=jax.ShapeDtypeStruct((2, PLAN), jnp.int32),
        in_specs=[smem] * 4,
        out_specs=smem,
        cost_estimate=pl.CostEstimate(flops=4_000_000, bytes_accessed=4_000, transcendentals=0),
        name="list_spans",
    )(where, dest, order, lengths)


def attention(plan, query_arrays, arrays, pieces):
    count = len(arrays)
    smem = pl.BlockSpec(memory_space=pltpu.SMEM)
    anywhere = pl.BlockSpec(memory_space=KEEP)
    rows = QUERIES_PER_KV * SPAN
    return pl.pallas_call(
        functools.partial(attention_kernel, pieces, count),
        out_shape=jax.ShapeDtypeStruct((2 * SPAN, QUERY_WIDTH), jnp.bfloat16),
        in_specs=[smem] + [anywhere] * (3 + count),
        out_specs=pl.BlockSpec(memory_space=KEEP),
        scratch_shapes=[
            pltpu.VMEM((2, SPAN, QUERY_WIDTH), jnp.bfloat16),
            pltpu.VMEM((SPANS * SPAN, HALF_WIDTH), jnp.bfloat16),
            pltpu.VMEM((SPANS * SPAN, HALF_WIDTH), jnp.bfloat16),
            pltpu.VMEM((MOST_CHUNKS, KEY_VALUE_HEADS, rows, CHUNK * SPAN), jnp.float32),
            pltpu.VMEM((KEY_VALUE_HEADS, rows, HEAD_SIZE), jnp.float32),
            pltpu.VMEM((KEY_VALUE_HEADS, rows, HEAD_SIZE), jnp.float32),
            pltpu.VMEM((KEY_VALUE_HEADS, rows, HEAD_SIZE), jnp.float32),
            pltpu.VMEM((2, SPAN, QUERY_WIDTH), jnp.bfloat16),
            pltpu.SemaphoreType.DMA((2,)),
            pltpu.SemaphoreType.DMA((SPANS, 2)),
            pltpu.SemaphoreType.DMA((2,)),
        ],
        cost_estimate=pl.CostEstimate(
            flops=1_000_000_000, bytes_accessed=4_000_000, transcendentals=2_000_000
        ),
        name="attend",
    )(plan, *query_arrays, *arrays)


def swaps(count, first):
    pairs = [(i % count, (i + 1) % count) for i in range(first, first + count, 2)]
    return pairs + [(b, a) for a, b in pairs]


def on_device(qkv, dest, order, lengths):
    dp_count = lax.axis_size("dp")
    dp_index = lax.axis_index("dp")
    column = lax.axis_index("ctx_0")
    row = lax.axis_index("ctx_1")
    columns = lax.axis_size("ctx_0")
    odd = dp_index & 1
    even_partner = dp_index + 1 - 2 * odd
    odd_partner = (dp_index - 1 + 2 * odd + dp_count) % dp_count
    resident = qkv[0]

    def trade(array, first):
        return lax.ppermute(array, "dp", swaps(dp_count, first))

    kv = resident[:, QUERY_WIDTH:]
    query_odd = trade(resident, 1)
    even_rows = trade(resident, 0)
    kv_odd = trade(kv, 1)
    kv_even = even_rows[:, QUERY_WIDTH:]
    own_sources = lax.dynamic_slice_in_dim(dest[0], 2 * (2 * column + row), 2)
    row_from = jnp.repeat(own_sources, SPAN)[:, None]
    own = jnp.where(
        row_from == even_partner, kv_even, jnp.where(row_from == odd_partner, kv_odd, kv)
    )
    other = lax.ppermute(own, "ctx_1", [(0, 1), (1, 0)])

    def across(array, first):
        return lax.ppermute(array, "ctx_0", swaps(columns, first))

    arrays = [own, other]
    ways = [0, 0]
    last = []
    for stream in (own, other):
        even, odd_side = stream, stream
        for step in range(1, 4):
            even, odd_side = across(odd_side, 0), across(even, 1)
            arrays += [even, odd_side]
            ways += [step, -step]
        last.append((even, odd_side))
    arrays += [across(last[0][1], 0), across(last[1][0], 1)]
    ways += [4, 4]
    flips = [0, 1] + [0] * 6 + [1] * 6 + [0, 1]
    pieces = [
        (index, part * SPAN, ways[index], flips[index], part)
        for index in range(len(arrays))
        for part in range(2)
    ]
    lane = jnp.arange(8, dtype=jnp.int32)
    where = jnp.where(
        lane == 0,
        dp_index,
        jnp.where(
            lane == 1,
            column,
            jnp.where(lane == 2, row, jnp.where(lane == 3, even_partner, odd_partner)),
        ),
    ).astype(jnp.int32)
    plan = list_key_spans(where, dest, order, lengths, pieces)
    attended = attention(plan, (resident, even_rows, query_odd), arrays, pieces)
    return attended[None]


def solution(mesh):
    finer = Mesh(mesh.devices.reshape(mesh.shape["dp"], 8, 2), ("dp", "ctx_0", "ctx_1"))
    placed = (P("dp", CTX, None), P("dp", None), P(), P())

    return jax.shard_map(
        on_device, mesh=finer, in_specs=placed, out_specs=P("dp", CTX, None), check_vma=False
    )
```

```python
import functools
import math

import jax
import jax.numpy as jnp
from jax import lax
from jax.experimental import pallas as pl
from jax.experimental.pallas import tpu as pltpu
from jax.sharding import Mesh
from jax.sharding import PartitionSpec as P


QUERY_HEADS = 32
KEY_VALUE_HEADS = 4
HEAD_SIZE = 128
NDOC = 8
SPAN = 64
QUERIES_PER_KV = 8
CTX = ("ctx_0", "ctx_1")
QUERY_WIDTH = QUERY_HEADS * HEAD_SIZE
HALF_WIDTH = KEY_VALUE_HEADS * HEAD_SIZE
SPANS = 32
CHUNK = 4
MOST_CHUNKS = 5
LISTED, BASES, WANTED = 0, 40, 80
ENDS, WHICH, POSITION, CHUNKS = 112, 120, 121, 122
PLAN = 128
KEEP = pl.ANY
FAR = 1 << 20
MASK_FLOOR = -1e30
EXP2_SCALE = math.log2(math.e) / math.sqrt(HEAD_SIZE)


def piece_slot(where_ref, piece):
    _, _, step, flip, part = piece
    column, row = where_ref[1], where_ref[2]
    there = (column + (1 - 2 * (column & 1)) * step) & 7
    return 2 * (2 * there + (row ^ flip)) + part


def list_kernel(pieces, where_ref, dest_ref, order_ref, lengths_ref, plan_ref):
    own_slot = 2 * (2 * where_ref[1] + where_ref[2])
    sources, spans, firsts = [], [], []
    for half in range(2):
        source = dest_ref[0, own_slot + half]
        plan_ref[half, WHICH] = jnp.where(
            source == where_ref[3], 1, jnp.where(source == where_ref[4], 2, 0)
        )
        span = order_ref[own_slot + half]
        plan_ref[half, POSITION] = span * SPAN
        end, first = jnp.int32(0), jnp.int32(0)
        for doc in range(NDOC):
            end = end + lengths_ref[source, doc]
            plan_ref[half, ENDS + doc] = end
            first = jnp.where(end <= span * SPAN, end, first)
        sources.append(source)
        spans.append(span)
        firsts.append(first)
    counts = [jnp.int32(0), jnp.int32(0)]
    for index, piece in enumerate(pieces):
        slot = piece_slot(where_ref, piece)
        source, span = dest_ref[0, slot], order_ref[slot]
        for half in range(2):
            need = (
                (source == sources[half])
                & (span <= spans[half])
                & (span * SPAN + SPAN > firsts[half])
            )
            plan_ref[half, LISTED + counts[half]] = index
            plan_ref[half, BASES + counts[half]] = span * SPAN
            need = need.astype(jnp.int32)
            plan_ref[half, WANTED + index] = need
            counts[half] = counts[half] + need
    for half in range(2):
        plan_ref[half, CHUNKS] = (counts[half] + CHUNK - 1) // CHUNK
        for extra in range(CHUNK - 1):
            plan_ref[half, LISTED + counts[half] + extra] = half
            plan_ref[half, BASES + counts[half] + extra] = FAR


def attention_kernel(pieces, count, *refs):
    plan = refs[0]
    query_refs = refs[1:4]
    piece_refs = refs[4 : 4 + count]
    out_ref = refs[4 + count]
    (queries, keys, values, scores, peaks, sums, mixed, outs, query_sems, piece_sems, out_sems) = refs[
        5 + count :
    ]

    def query_copy(half, which):
        rows = pl.ds(half * SPAN, SPAN)
        return pltpu.make_async_copy(
            query_refs[which].at[rows, pl.ds(0, QUERY_WIDTH)],
            queries.at[half],
            query_sems.at[half],
        )

    def out_copy(half):
        return pltpu.make_async_copy(
            outs.at[half], out_ref.at[pl.ds(half * SPAN, SPAN)], out_sems.at[half]
        )

    def piece_copies(index):
        ref, first_row = pieces[index][0], pieces[index][1]
        rows = pl.ds(first_row, SPAN)
        there = pl.ds(index * SPAN, SPAN)
        return (
            pltpu.make_async_copy(
                piece_refs[ref].at[rows, pl.ds(0, HALF_WIDTH)], keys.at[there], piece_sems.at[index, 0]
            ),
            pltpu.make_async_copy(
                piece_refs[ref].at[rows, pl.ds(HALF_WIDTH, HALF_WIDTH)],
                values.at[there],
                piece_sems.at[index, 1],
            ),
        )

    def for_wanted(act):
        for index in range(SPANS):

            @pl.when(plan[0, WANTED + index] + plan[1, WANTED + index] > 0)
            def _(index=index):
                act(piece_copies(index))

    for half in range(2):
        for which in range(3):

            @pl.when(plan[half, WHICH] == which)
            def _(half=half, which=which):
                query_copy(half, which).start()

        for_wanted(lambda copies: copies[half].start())

    lane = lax.broadcasted_iota(jnp.int32, (1, CHUNK * SPAN), 1)
    rows = QUERIES_PER_KV * SPAN

    def one_half(half, unused):
        position = plan[half, POSITION] + lax.broadcasted_iota(jnp.int32, (SPAN, 1), 0)
        start = jnp.zeros((SPAN, 1), jnp.int32)
        for doc in range(NDOC):
            end = plan[half, ENDS + doc]
            start = jnp.where(position >= end, end, start)
        chunks = plan[half, CHUNKS]
        peaks[...] = jnp.full_like(peaks, MASK_FLOOR)
        sums[...] = jnp.zeros_like(sums)
        mixed[...] = jnp.zeros_like(mixed)
        query_copy(half, 0).wait()

        @pl.when(half == 0)
        def _():
            for_wanted(lambda copies: copies[0].wait())

        def first_rows(chunk):
            return [
                pl.multiple_of(plan[half, LISTED + chunk * CHUNK + j] * SPAN, SPAN)
                for j in range(CHUNK)
            ]

        def score_chunk(chunk, carry):
            at = BASES + chunk * CHUNK
            base = jnp.full((1, CHUNK * SPAN), plan[half, at], jnp.int32)
            for j in range(1, CHUNK):
                base = jnp.where(lane >= j * SPAN, plan[half, at + j], base)
            key_position = (lane & (SPAN - 1)) + base
            visible = (key_position <= position) & (key_position >= start)
            bias = jnp.where(visible, 0.0, MASK_FLOOR).astype(jnp.float32)
            firsts_of = first_rows(chunk)
            for group in range(KEY_VALUE_HEADS):
                columns = slice(group * HEAD_SIZE, (group + 1) * HEAD_SIZE)
                key = jnp.concatenate([keys[pl.ds(f, SPAN), columns] for f in firsts_of], axis=0)
                query = jnp.concatenate(
                    [
                        queries[half, :, pl.ds((group * QUERIES_PER_KV + h) * HEAD_SIZE, HEAD_SIZE)]
                        for h in range(QUERIES_PER_KV)
                    ],
                    axis=0,
                )
                score = lax.dot_general(
                    query, key, (((1,), (1,)), ((), ())), preferred_element_type=jnp.float32
                )
                score = score.reshape(QUERIES_PER_KV, SPAN, CHUNK * SPAN) * EXP2_SCALE + bias[None]
                score = score.reshape(rows, CHUNK * SPAN)
                scores[chunk, group] = score
                peak = peaks[group]
                for j in range(0, CHUNK * SPAN, HEAD_SIZE):
                    peak = jnp.maximum(peak, score[:, j : j + HEAD_SIZE])
                peaks[group] = peak
            return carry

        lax.fori_loop(0, chunks, score_chunk, 0)
        for group in range(KEY_VALUE_HEADS):
            peaks[group] = jnp.broadcast_to(
                jnp.max(peaks[group], axis=1, keepdims=True), (rows, HEAD_SIZE)
            )

        @pl.when(half == 0)
        def _():
            for_wanted(lambda copies: copies[1].wait())

        def mix_chunk(chunk, carry):
            firsts_of = first_rows(chunk)
            for group in range(KEY_VALUE_HEADS):
                columns = slice(group * HEAD_SIZE, (group + 1) * HEAD_SIZE)
                value = jnp.concatenate([values[pl.ds(f, SPAN), columns] for f in firsts_of], axis=0)
                peak = peaks[group]
                total = sums[group]
                weights = []
                for j in range(0, CHUNK * SPAN, HEAD_SIZE):
                    weight = jnp.exp2(scores[chunk, group, :, j : j + HEAD_SIZE] - peak)
                    total = total + weight
                    weights.append(weight.astype(jnp.bfloat16))
                sums[group] = total
                mixed[group] += jnp.dot(
                    jnp.concatenate(weights, axis=1), value, preferred_element_type=jnp.float32
                )
            return carry

        lax.fori_loop(0, chunks, mix_chunk, 0)
        for group in range(KEY_VALUE_HEADS):
            total = jnp.sum(sums[group], axis=1, keepdims=True)
            result = (mixed[group] * (1.0 / total)).astype(jnp.bfloat16)
            for h in range(QUERIES_PER_KV):
                outs[half, :, pl.ds((group * QUERIES_PER_KV + h) * HEAD_SIZE, HEAD_SIZE)] = result[
                    h * SPAN : (h + 1) * SPAN
                ]
        out_copy(half).start()
        return unused

    lax.fori_loop(0, 2, one_half, 0)
    for half in range(2):
        out_copy(half).wait()


def list_key_spans(where, dest, order, lengths, pieces):
    smem = pl.BlockSpec(memory_space=pltpu.SMEM)
    return pl.pallas_call(
        functools.partial(list_kernel, pieces),
        out_shape=jax.ShapeDtypeStruct((2, PLAN), jnp.int32),
        in_specs=[smem] * 4,
        out_specs=smem,
        cost_estimate=pl.CostEstimate(flops=4_000_000, bytes_accessed=4_000, transcendentals=0),
        name="list_spans",
    )(where, dest, order, lengths)


def attention(plan, query_arrays, arrays, pieces):
    count = len(arrays)
    smem = pl.BlockSpec(memory_space=pltpu.SMEM)
    anywhere = pl.BlockSpec(memory_space=KEEP)
    rows = QUERIES_PER_KV * SPAN
    return pl.pallas_call(
        functools.partial(attention_kernel, pieces, count),
        out_shape=jax.ShapeDtypeStruct((2 * SPAN, QUERY_WIDTH), jnp.bfloat16),
        in_specs=[smem] + [anywhere] * (3 + count),
        out_specs=pl.BlockSpec(memory_space=KEEP),
        scratch_shapes=[
            pltpu.VMEM((2, SPAN, QUERY_WIDTH), jnp.bfloat16),
            pltpu.VMEM((SPANS * SPAN, HALF_WIDTH), jnp.bfloat16),
            pltpu.VMEM((SPANS * SPAN, HALF_WIDTH), jnp.bfloat16),
            pltpu.VMEM((MOST_CHUNKS, KEY_VALUE_HEADS, rows, CHUNK * SPAN), jnp.float32),
            pltpu.VMEM((KEY_VALUE_HEADS, rows, HEAD_SIZE), jnp.float32),
            pltpu.VMEM((KEY_VALUE_HEADS, rows, HEAD_SIZE), jnp.float32),
            pltpu.VMEM((KEY_VALUE_HEADS, rows, HEAD_SIZE), jnp.float32),
            pltpu.VMEM((2, SPAN, QUERY_WIDTH), jnp.bfloat16),
            pltpu.SemaphoreType.DMA((2,)),
            pltpu.SemaphoreType.DMA((SPANS, 2)),
            pltpu.SemaphoreType.DMA((2,)),
        ],
        cost_estimate=pl.CostEstimate(
            flops=1_000_000_000, bytes_accessed=4_000_000, transcendentals=2_000_000
        ),
        name="attend",
    )(plan, *query_arrays, *arrays)


def swaps(count, first):
    pairs = [(i % count, (i + 1) % count) for i in range(first, first + count, 2)]
    return pairs + [(b, a) for a, b in pairs]


def on_device(qkv, dest, order, lengths):
    dp_count = lax.axis_size("dp")
    dp_index = lax.axis_index("dp")
    column = lax.axis_index("ctx_0")
    row = lax.axis_index("ctx_1")
    columns = lax.axis_size("ctx_0")
    odd = dp_index & 1
    even_partner = dp_index + 1 - 2 * odd
    odd_partner = (dp_index - 1 + 2 * odd + dp_count) % dp_count
    resident = qkv[0]

    def trade(array, first):
        return lax.ppermute(array, "dp", swaps(dp_count, first))

    kv = resident[:, QUERY_WIDTH:]
    query_odd = trade(resident, 1)
    even_rows = trade(resident, 0)
    kv_even = trade(kv, 0)
    kv_odd = trade(kv, 1)
    own_sources = lax.dynamic_slice_in_dim(dest[0], 2 * (2 * column + row), 2)
    row_from = jnp.repeat(own_sources, SPAN)[:, None]
    own = jnp.where(
        row_from == even_partner, kv_even, jnp.where(row_from == odd_partner, kv_odd, kv)
    )
    other = lax.ppermute(own, "ctx_1", [(0, 1), (1, 0)])

    def across(array, first):
        return lax.ppermute(array, "ctx_0", swaps(columns, first))

    arrays = [own, other]
    ways = [0, 0]
    last = []
    for stream in (own, other):
        even, odd_side = stream, stream
        for step in range(1, 4):
            next_even = across(odd_side, 0)
            odd_side = across(even, 1)
            even = next_even
            arrays += [even, odd_side]
            ways += [step, -step]
        last.append((even, odd_side))
    arrays.append(across(last[0][1], 0))
    arrays.append(across(last[1][0], 1))
    ways += [4, 4]
    flips = [0, 1] + [0] * 6 + [1] * 6 + [0, 1]
    pieces = [
        (index, part * SPAN, ways[index], flips[index], part)
        for index in range(len(arrays))
        for part in range(2)
    ]
    lane = jnp.arange(8, dtype=jnp.int32)
    where = jnp.where(
        lane == 0,
        dp_index,
        jnp.where(
            lane == 1,
            column,
            jnp.where(lane == 2, row, jnp.where(lane == 3, even_partner, odd_partner)),
        ),
    ).astype(jnp.int32)
    plan = list_key_spans(where, dest, order, lengths, pieces)
    attended = attention(plan, (resident, even_rows, query_odd), arrays, pieces)
    return attended[None]


def solution(mesh):
    finer = Mesh(mesh.devices.reshape(mesh.shape["dp"], 8, 2), ("dp", "ctx_0", "ctx_1"))
    placed = (P("dp", CTX, None), P("dp", None), P(), P())

    return jax.shard_map(
        on_device, mesh=finer, in_specs=placed, out_specs=P("dp", CTX, None), check_vma=False
    )
```
